32 devices in a mesh: fit: 2 (over x), comp: 4 (over z), data: 4 (over y, core).
Axes of the slice: x: 2, y: 2, z: 4, core: 2. Of those that a mesh axis runs over, the one named last changes fastest.
Arguments:
- points: bfloat16 [8192, 256], P(('fit', 'data')), parts along dimension 0
- mu_init: float32 [32768, 256], P(('fit', 'comp')), parts along dimension 0
- logpi_init: float32 [32768], P(('fit', 'comp')), parts along dimension 0
- inv_temp: float32 [3], replicated
Outputs:
- output 1: float32 [32768, 256], P(('fit', 'comp', 'data')), parts along dimension 0
- output 2: float32 [32768], P(('fit', 'comp', 'data')), parts along dimension 0
- output 3: float32 [8192], P(('fit', 'data')), parts along dimension 0
There are 2 independent parts. The reference program is written for one: setup_inputs(seed, part) draws one part's arguments, and reference() takes and returns one part's arrays. A program takes and returns all parts, laid end to end along the dimension named above; an argument that names none is the same for every part.
All inputs are finite; a program needn't handle non-finite values.
Results may differ from the reference program's by a relative error of at most 0.00362.
Values are sent between devices in bfloat16 or wider.
A program may use at most 1 GiB of HBM per device.

```python
import math
import jax
import jax.numpy as jnp
from jax import lax

N = 4096
K = 16384
D = 256
SWEEPS = 3
SOURCES = 64
ROW_BLK = math.gcd(N, max(8, 2 ** 23 // K))
MEAN_EPS = 1e-6
PRIOR_ALPHA = 1e-3


def setup_inputs(seed: int = 0, part: int = 0) -> dict:
    root_key = jax.random.key(seed)
    part_root, key_temp = jax.random.split(root_key)
    part_key = jax.random.fold_in(part_root, part)
    key_cent, key_noise, key_src, key_mu, key_pi = jax.random.split(part_key, 5)
    unit_scale = D ** -0.5
    centres = jax.random.normal(key_cent, (SOURCES, D), jnp.float32) * unit_scale
    source_id = (jnp.arange(N) * SOURCES) // N
    point_noise = jax.random.normal(key_noise, (N, D), jnp.float32) * (0.8 * unit_scale)
    points = (centres[source_id] + point_noise).astype(jnp.bfloat16)
    comp_source = jax.random.randint(key_src, (K,), 0, SOURCES)
    mu_init = centres[comp_source] + jax.random.normal(key_mu, (K, D), jnp.float32) * (0.8 * unit_scale)
    raw_pi = jax.random.normal(key_pi, (K,), jnp.float32)
    logpi_init = raw_pi - jax.nn.logsumexp(raw_pi)
    temp_ramp = jnp.power(1.6, jnp.arange(SWEEPS).astype(jnp.float32))
    inv_temp = jax.random.uniform(key_temp, (SWEEPS,), jnp.float32, 0.4, 0.7) * (D ** 0.5) * temp_ramp
    return {'points': points, 'mu_init': mu_init, 'logpi_init': logpi_init, 'inv_temp': inv_temp}


def responsibilities(x_blk, sq_blk, mu_bf, mu_sq, log_wts, beta_t):
    cross_dot = jnp.dot(x_blk, mu_bf.T, preferred_element_type=jnp.float32)
    logits = log_wts[None, :] - beta_t * (sq_blk[:, None] - 2.0 * cross_dot + mu_sq[None, :])
    row_max = jnp.max(logits, axis=1)
    row_sum = jnp.sum(jnp.exp(logits - row_max[:, None]), axis=1)
    log_norm = row_max + jnp.log(row_sum)
    return jnp.exp(logits - log_norm[:, None]), log_norm


def reference(points, mu_init, logpi_init, inv_temp):
    n_blocks = N // ROW_BLK
    x_blocks = points.reshape(n_blocks, ROW_BLK, D)
    pt_sq = jnp.sum(jnp.square(points.astype(jnp.float32)), axis=1).reshape(n_blocks, ROW_BLK)

    def sweep(state_in, beta_t):
        means, log_wts = state_in
        mu_bf = means.astype(jnp.bfloat16)
        mu_sq = jnp.sum(means * means, axis=1)

        def block_step(running, block_in):
            x_blk, sq_blk = block_in
            respons, log_norm = responsibilities(x_blk, sq_blk, mu_bf, mu_sq, log_wts, beta_t)
            stat_blk = jnp.dot(respons.astype(jnp.bfloat16).T, x_blk, preferred_element_type=jnp.float32)
            return (running[0] + stat_blk, running[1] + jnp.sum(respons, axis=0)), log_norm

        zero_sums = (jnp.zeros((K, D), jnp.float32), jnp.zeros((K,), jnp.float32))
        (stat_sum, counts), log_norm = lax.scan(block_step, zero_sums, (x_blocks, pt_sq))
        new_means = stat_sum / (counts[:, None] + MEAN_EPS)
        new_wts = jnp.log((counts + PRIOR_ALPHA) / (N + K * PRIOR_ALPHA))
        return (new_means, new_wts), log_norm.reshape(N)

    (means, log_pi), all_norms = lax.scan(sweep, (mu_init, logpi_init), inv_temp)
    return means, log_pi, all_norms[-1]
```

```python
import functools
import math

import jax
import jax.numpy as jnp
from jax import lax
from jax.experimental import pallas as pl
from jax.experimental.pallas import tpu as pltpu
from jax.sharding import PartitionSpec as P

MEAN_EPS = 1e-6
PRIOR_ALPHA = 1e-3
LOG2E = math.log2(math.e)
LN2 = math.log(2.0)
F32 = jnp.float32
BF16 = jnp.bfloat16
MESH = pl.DeviceIdType.MESH
NT = (((1,), (1,)), ((), ()))
T = 256
RB = 64


def em_kernel(
    n_sweeps, n_total,
    beta_ref, x_hbm, mu_hbm, lp_hbm,
    out_mu, out_lp, out_lse,
    x_all, mu_f, lp_v, mu_bf, cvec, eb, mb, sb0, sb1, lam, lam_all, s1_buf, s2_buf, nacc, rbuf, s_acc,
    loc_sem, xs_send, xs_recv, s1_send, s1_recv, s2_send, s2_recv,
):
    n_pts = x_all.shape[0]
    n_loc = x_hbm.shape[0]
    k_loc = mu_f.shape[0]
    n_tiles = n_pts // T
    tiles_blk = n_loc // T
    nb = k_loc // RB
    rows_blk = n_loc // 128
    half_rows = lam.shape[1]
    f_i, z_i, d_i = lax.axis_index("fit"), lax.axis_index("comp"), lax.axis_index("data")
    nz, nd = 4, 4
    sib = d_i + 1 - 2 * lax.rem(d_i, 2)
    ypeer = lax.rem(d_i + 2, nd)
    cross = lax.rem(sib + 2, nd)
    quad = [sib, ypeer, cross]
    zs = [lax.rem(z_i + k, nz) for k in (1, 2, 3)]

    def dev(z, d):
        return (f_i, z, d)

    def rcopy(src, dst, ssem, rsem, device):
        return pltpu.make_async_remote_copy(
            src_ref=src, dst_ref=dst, send_sem=ssem, recv_sem=rsem, device_id=device, device_id_type=MESH
        )

    barrier = pltpu.get_barrier_semaphore()
    for q in quad:
        pl.semaphore_signal(barrier, inc=1, device_id=dev(z_i, q), device_id_type=MESH)
    for z in zs:
        pl.semaphore_signal(barrier, inc=1, device_id=dev(z, d_i), device_id_type=MESH)

    def blk_rows(b):
        return pl.ds(pl.multiple_of(b * n_loc, n_loc), n_loc)

    cp_x = pltpu.make_async_copy(x_hbm, x_all.at[blk_rows(d_i), :], loc_sem.at[0])
    cp_mu = pltpu.make_async_copy(mu_hbm.at[pl.ds(pl.multiple_of(d_i * k_loc, k_loc), k_loc), :], mu_f, loc_sem.at[1])
    cp_lp = pltpu.make_async_copy(lp_hbm.at[pl.ds(pl.multiple_of(d_i * rows_blk, rows_blk), rows_blk), :], lp_v, loc_sem.at[2])
    cp_x.start()
    cp_mu.start()
    cp_lp.start()
    cp_x.wait()
    pl.semaphore_wait(barrier, 6)
    x_sib = rcopy(x_all.at[blk_rows(d_i), :], x_all.at[blk_rows(d_i), :], xs_send.at[0], xs_recv.at[0], dev(z_i, sib))
    x_sib.start()

    def piece(b, p):
        return x_all.at[pl.ds(pl.multiple_of(b * n_loc + p * T, T), T), :]

    x_y = []
    for p in range(tiles_blk):
        c = rcopy(piece(d_i, p), piece(d_i, p), xs_send.at[1 + p], xs_recv.at[1 + p], dev(z_i, ypeer))
        c.start()
        x_y.append(c)
    cp_mu.wait()
    cp_lp.wait()

    eye = lax.broadcasted_iota(jnp.int32, (128, 128), 0) == lax.broadcasted_iota(jnp.int32, (128, 128), 1)

    bp0 = beta_ref[0] * LOG2E
    for g in range(k_loc // 128):
        r = slice(g * 128, (g + 1) * 128)
        m = mu_f[r, :]
        mu_bf[r, :] = m.astype(BF16)
        sq = m * m
        w = jnp.where(eye, lp_v[g : g + 1, :] * LOG2E, 0.0) - bp0 * (sq[:, :128] + sq[:, 128:])
        cvec[r, :] = jnp.broadcast_to(jnp.sum(w, axis=1, keepdims=True), (128, 128))

    def e_pair(tiles, b2):
        sbs = (sb0, sb1)
        logits = []
        for q in range(2):
            xt = x_all[pl.ds(pl.multiple_of(tiles[q] * T, T), T), :]
            logits.append(lax.dot_general(mu_bf[...], xt, NT, preferred_element_type=F32))
        for j in range(nb):
            r = slice(j * RB, (j + 1) * RB)
            for q in range(2):
                cc = cvec[r, :]
                l3 = (logits[q][r] * b2 + jnp.concatenate([cc, cc], axis=1)).reshape(RB // 8, 8, T)
                m = jnp.max(l3, axis=0)
                e = jnp.exp2(l3 - m[None])
                eb[tiles[q], r, :] = e.reshape(RB, T)
                mb[tiles[q], j] = m
                sbs[q][j] = jnp.sum(e, axis=0)
        for q in range(2):
            t = tiles[q]
            mx = mb[t, 0]
            for j in range(1, nb):
                mx = jnp.maximum(mx, mb[t, j])
            mx = jnp.max(mx, axis=0, keepdims=True)
            s = sbs[q][0] * jnp.exp2(mb[t, 0] - mx)
            for j in range(1, nb):
                s = s + sbs[q][j] * jnp.exp2(mb[t, j] - mx)
            lm = mx + jnp.log2(jnp.sum(s, axis=0, keepdims=True))
            per_half = n_tiles // 2
            h = t // per_half
            tl = lax.rem(t, per_half)
            lam[h, pl.ds(2 * tl, 1), :] = lm[:, :128]
            lam[h, pl.ds(2 * tl + 1, 1), :] = lm[:, 128:]

    def s1_start(s, h):
        cs = []
        for k, q in enumerate(quad):
            c = rcopy(lam.at[h], s1_buf.at[s, h, d_i], s1_send.at[s, h, k], s1_recv.at[s, h, d_i], dev(z_i, q))
            c.start()
            cs.append(c)
        return cs

    def lse4(vals):
        mx = functools.reduce(jnp.maximum, vals)
        tot = functools.reduce(lambda a, b: a + b, [jnp.exp2(v - mx) for v in vals])
        return mx + jnp.log2(tot)

    def s1_finish(s, h):
        for q in quad:
            rcopy(lam.at[h], s1_buf.at[s, h, q], s1_send.at[s, h, 0], s1_recv.at[s, h, q], dev(z_i, q)).wait_recv()
        v = lse4([lam[h]] + [s1_buf[s, h, q] for q in quad])
        s2_buf[s, h, z_i] = v

    def s2_start(s, h):
        cs = []
        for k, z in enumerate(zs):
            c = rcopy(s2_buf.at[s, h, z_i], s2_buf.at[s, h, z_i], s2_send.at[s, h, k], s2_recv.at[s, h, z_i], dev(z, d_i))
            c.start()
            cs.append(c)
        return cs

    def s2_finish(s, h):
        for z in zs:
            rcopy(s2_buf.at[s, h, z], s2_buf.at[s, h, z], s2_send.at[s, h, 0], s2_recv.at[s, h, z], dev(z, d_i)).wait_recv()
        lam_all[h * half_rows : (h + 1) * half_rows, :] = lse4([s2_buf[s, h, z] for z in range(nz)])

    def m_half(h):
        per_chunk = rbuf.shape[1] // T

        def chunk(i, _):
            t0 = h * (n_tiles // 2) + i * per_chunk
            for k in range(per_chunk):
                t = t0 + k
                lrow = jnp.concatenate([lam_all[pl.ds(2 * t, 1), :], lam_all[pl.ds(2 * t + 1, 1), :]], axis=1)
                for b in range(nb):
                    r = slice(b * RB, (b + 1) * RB)
                    fac = jnp.exp2(mb[t, b] - lrow)
                    rv = (eb[t, r, :].reshape(RB // 8, 8, T) * fac[None]).reshape(RB, T)
                    nacc[r, :] += rv[:, :128] + rv[:, 128:]
                    rbuf[r, k * T : (k + 1) * T] = rv.astype(BF16)
            xt = x_all[pl.ds(pl.multiple_of(t0 * T, T), per_chunk * T), :]
            s_acc[...] += jnp.dot(rbuf[...], xt, preferred_element_type=F32)
            return 0

        lax.fori_loop(0, n_tiles // 2 // per_chunk, chunk, 0)

    def update(s):
        last = s + 1 == n_sweeps
        inv_tot = 1.0 / (n_pts + n_total * PRIOR_ALPHA)
        if not last:
            bp = beta_ref[s + 1] * LOG2E
        for b in range(nb):
            r = slice(b * RB, (b + 1) * RB)
            st = s_acc[r, :]
            n = jnp.sum(nacc[r, :], axis=1, keepdims=True)
            mu = st * (1.0 / (n + MEAN_EPS))
            l2 = jnp.log2((n + PRIOR_ALPHA) * inv_tot)
            if last:
                out_mu[r, :] = mu
                cvec[r, :] = jnp.broadcast_to(l2 * LN2, (RB, 128))
            else:
                mu_bf[r, :] = mu.astype(BF16)
                sq = mu * mu
                p = jnp.sum(sq[:, :128] + sq[:, 128:], axis=1, keepdims=True)
                cvec[r, :] = jnp.broadcast_to(l2 - bp * p, (RB, 128))
        if last:
            for g in range(k_loc // 128):
                out_lp[g : g + 1, :] = jnp.sum(jnp.where(eye, cvec[g * 128 : (g + 1) * 128, :], 0.0), axis=0, keepdims=True)

    for s in range(n_sweeps):
        b2 = beta_ref[s] * (2.0 * LOG2E)
        nacc[...] = jnp.zeros_like(nacc)
        s_acc[...] = jnp.zeros_like(s_acc)
        sends = []
        if s == 0:
            def own(i, _):
                t = d_i * tiles_blk + 2 * i
                e_pair((t, t + 1), b2)
                return 0

            lax.fori_loop(0, tiles_blk // 2, own, 0)
            rcopy(x_all.at[blk_rows(sib), :], x_all.at[blk_rows(sib), :], xs_send.at[0], xs_recv.at[0], dev(z_i, sib)).wait_recv()

            def sibl(i, _):
                t = sib * tiles_blk + 2 * i
                e_pair((t, t + 1), b2)
                return 0

            lax.fori_loop(0, tiles_blk // 2, sibl, 0)
            fwd = []

            def take(p):
                rcopy(piece(ypeer, p), piece(ypeer, p), xs_send.at[1 + p], xs_recv.at[1 + p], dev(z_i, ypeer)).wait_recv()
                c = rcopy(piece(ypeer, p), piece(ypeer, p), xs_send.at[1 + tiles_blk + p], xs_recv.at[1 + tiles_blk + p], dev(z_i, sib))
                c.start()
                fwd.append(c)

            take(0)
            for p in range(tiles_blk):
                if p + 1 < tiles_blk:
                    take(p + 1)
                rcopy(piece(cross, p), piece(cross, p), xs_send.at[1 + tiles_blk + p], xs_recv.at[1 + tiles_blk + p], dev(z_i, sib)).wait_recv()
                e_pair((ypeer * tiles_blk + p, cross * tiles_blk + p), b2)
            sends += s1_start(s, 0) + s1_start(s, 1)
            x_sib.wait_send()
            for c in x_y + fwd:
                c.wait_send()
            s1_finish(s, 0)
            sends += s2_start(s, 0)
            s1_finish(s, 1)
            sends += s2_start(s, 1)
        else:
            for h in range(2):
                def body(i, _, h=h):
                    t = h * (n_tiles // 2) + 2 * i
                    e_pair((t, t + 1), b2)
                    return 0

                lax.fori_loop(0, n_tiles // 4, body, 0)
                sends += s1_start(s, h)
            for h in range(2):
                s1_finish(s, h)
                sends += s2_start(s, h)
        if s + 1 == n_sweeps:
            for g in range(rows_blk):
                xf = x_all[pl.ds(pl.multiple_of(d_i * n_loc + g * 128, 128), 128), :].astype(F32)
                sq = xf * xf
                qc = jnp.sum(sq[:, :128] + sq[:, 128:], axis=1, keepdims=True)
                lp_v[g : g + 1, :] = jnp.sum(jnp.where(eye, qc, 0.0), axis=0, keepdims=True)
        for h in range(2):
            s2_finish(s, h)
            m_half(h)
        for c in sends:
            c.wait_send()
        update(s)
    out_lse[...] = lam_all[pl.ds(pl.multiple_of(d_i * rows_blk, rows_blk), rows_blk), :] * LN2 - beta_ref[n_sweeps - 1] * lp_v[...]


def solution(mesh):
    n_comp_dev = mesh.shape["comp"]
    n_data_dev = mesh.shape["data"]

    def local_fit(points, mu_init, logpi_init, inv_temp):
        n_loc, dim = points.shape
        k_all = mu_init.shape[0]
        n_pts = n_loc * n_data_dev
        k_loc = k_all // n_data_dev
        n_total = k_all * n_comp_dev
        n_sweeps = inv_temp.shape[0]
        n_tiles = n_pts // T
        nb = k_loc // RB
        half_rows = n_pts // 256
        dma = pltpu.SemaphoreType.DMA
        vmem = pl.BlockSpec(memory_space=pltpu.VMEM)
        hbm = pl.BlockSpec(memory_space=pl.ANY)
        tiles_blk = n_loc // T
        means, log_pi, log_norm = pl.pallas_call(
            functools.partial(em_kernel, n_sweeps, n_total),
            out_shape=(
                jax.ShapeDtypeStruct((k_loc, dim), F32),
                jax.ShapeDtypeStruct((k_loc // 128, 128), F32),
                jax.ShapeDtypeStruct((n_loc // 128, 128), F32),
            ),
            in_specs=[pl.BlockSpec(memory_space=pltpu.SMEM), hbm, hbm, hbm],
            out_specs=(vmem, vmem, vmem),
            scratch_shapes=[
                pltpu.VMEM((n_pts, dim), BF16),
                pltpu.VMEM((k_loc, dim), F32),
                pltpu.VMEM((k_loc // 128, 128), F32),
                pltpu.VMEM((k_loc, dim), BF16),
                pltpu.VMEM((k_loc, 128), F32),
                pltpu.VMEM((n_tiles, k_loc, T), F32),
                pltpu.VMEM((n_tiles, nb, 8, T), F32),
                pltpu.VMEM((nb, 8, T), F32),
                pltpu.VMEM((nb, 8, T), F32),
                pltpu.VMEM((2, half_rows, 128), F32),
                pltpu.VMEM((2 * half_rows, 128), F32),
                pltpu.VMEM((n_sweeps, 2, 4, half_rows, 128), F32),
                pltpu.VMEM((n_sweeps, 2, 4, half_rows, 128), F32),
                pltpu.VMEM((k_loc, 128), F32),
                pltpu.VMEM((k_loc, min(n_pts // 2, 4 * T)), BF16),
                pltpu.VMEM((k_loc, dim), F32),
                dma((3,)),
                dma((1 + 2 * tiles_blk,)),
                dma((1 + 2 * tiles_blk,)),
                dma((n_sweeps, 2, 3)),
                dma((n_sweeps, 2, 4)),
                dma((n_sweeps, 2, 3)),
                dma((n_sweeps, 2, 4)),
            ],
            compiler_params=pltpu.CompilerParams(
                collective_id=0, has_side_effects=True, vmem_limit_bytes=60 * 2**20
            ),
            name="em_sweeps",
        )(inv_temp, points, mu_init, logpi_init.reshape(k_all // 128, 128))
        return means, log_pi.reshape(k_loc), log_norm.reshape(n_loc)

    return jax.shard_map(
        local_fit,
        mesh=mesh,
        in_specs=(P(("fit", "data"), None), P(("fit", "comp"), None), P(("fit", "comp")), P(None)),
        out_specs=(P(("fit", "comp", "data"), None), P(("fit", "comp", "data")), P(("fit", "data"))),
        check_vma=False,
    )
```
